256 devices in a mesh: dp: 32 (over y, z), rows: 8 (over x, core).
Axes of the slice: x: 4, y: 4, z: 8, core: 2. Of those that a mesh axis runs over, the one named last changes fastest.
Arguments:
- latent: float32 [32, 128, 32, 128], P('dp', 'rows'), may hold values from -12 to 12
- bits1: int32 [32, 16, 32, 16], P('dp', 'rows'), may hold values from -1 to 1, as said below
- bits2: int32 [32, 32, 32, 32], P('dp', 'rows'), may hold values from -1 to 1, as said below
- bits3: int32 [32, 64, 32, 64], P('dp', 'rows'), may hold values from -1 to 1, as said below
- bits4: int32 [32, 128, 32, 128], P('dp', 'rows'), may hold values from -1 to 1, as said below
- w_in: bfloat16 [3, 3, 32, 256], replicated, may hold values from -0.375 to 0.375
- w_mid: bfloat16 [3, 3, 256, 256], replicated, may hold values from -0.125 to 0.125
- w_out: bfloat16 [3, 3, 32, 256], replicated, may hold values from -0.125 to 0.125
Outputs:
- recon: float32 [32, 128, 32, 128], P('dp', 'rows')
- usage_entropy: float32 [4, 8], replicated
- sample_entropy: float32 [4], replicated
The draws below stay inside these ranges and needn't reach their ends.
Inputs may be any that keep to these rules, and one draw needn't show every extreme that they name: `bits1`: each entry is -1 or +1. `bits2`: each entry is -1 or +1. `bits3`: each entry is -1 or +1. `bits4`: each entry is -1 or +1.
All inputs are finite; a program needn't handle non-finite values.
Results may differ from the reference program's by a relative error of at most 0.0021.
Values may be sent and summed in bfloat16 or wider, within the bound.
A program may use at most 64 MiB of HBM per device.

```python
import math
from functools import partial
import jax
import jax.numpy as jnp
from jax import lax

H = 128
C = 32
HID = 256
GB = 4
B = 32
S1 = 16
S2 = 32
S3 = 64


def draw_latent(key, part):
    key_scale = jax.random.fold_in(key, 101)
    key_noise = jax.random.fold_in(key, 202)
    key_strength = jax.random.fold_in(key, 404)
    key_shared = jax.random.fold_in(key, 505)
    key_sign = jax.random.fold_in(key, 606)
    key_offset = jax.random.fold_in(key, 707)
    key_channel = jax.random.fold_in(key, 808)
    group_count = C // GB
    scales = jnp.exp(jax.random.uniform(key_scale, (B, H, 1, 1), minval=math.log(0.3), maxval=math.log(3.0)))
    strength = jnp.exp(jax.random.uniform(key_strength, (B, 1, group_count, 1, 1), minval=math.log(0.8), maxval=math.log(2.0)))
    image_sign = (2 * jax.random.randint(key_sign, (B, 1, C, 1), 0, 2) - 1).astype(jnp.float32)
    channel_sign = (2 * jax.random.randint(key_channel, (1, 1, C, 1), 0, 2) - 1).astype(jnp.float32)
    offset_size = jnp.exp(jax.random.uniform(key_offset, (B, 1, C, 1), minval=math.log(0.03), maxval=math.log(0.4)))
    offset = image_sign * offset_size + 0.15 * channel_sign
    noise = jnp.clip(jax.random.normal(key_noise, (B, H, C, H)), -3.0, 3.0)
    shared = jnp.clip(jax.random.normal(key_shared, (B, H, group_count, 1, H)), -3.0, 3.0)
    grouped = jnp.broadcast_to(strength * shared, (B, H, group_count, GB, H)).reshape(B, H, C, H)
    values = noise + grouped + offset
    return jnp.clip(scales * values, -12.0, 12.0).astype(jnp.float32)


def sign_draw(key, grid_side):
    coin_flips = jax.random.randint(key, (B, grid_side, C, grid_side), 0, 2)
    return (2 * coin_flips - 1).astype(jnp.int32)


def draw_bits1(key, part):
    return sign_draw(jax.random.fold_in(key, 11), S1)


def draw_bits2(key, part):
    return sign_draw(jax.random.fold_in(key, 12), S2)


def draw_bits3(key, part):
    return sign_draw(jax.random.fold_in(key, 13), S3)


def draw_bits4(key, part):
    return sign_draw(jax.random.fold_in(key, 14), H)


def normal_values(rng, extent, spread, limit, held_as=jnp.bfloat16):
    return jnp.clip(spread * jax.random.normal(rng, extent, jnp.float32), -limit, limit).astype(held_as)


def setup_inputs(seed: int = 0) -> dict:
    arg_keys = jax.random.split(jax.random.key(seed), 9)
    latent = draw_latent(jax.random.fold_in(arg_keys[8], 71), 0)
    bits1 = draw_bits1(jax.random.fold_in(arg_keys[8], 71), 0)
    bits2 = draw_bits2(jax.random.fold_in(arg_keys[8], 71), 0)
    bits3 = draw_bits3(jax.random.fold_in(arg_keys[8], 71), 0)
    bits4 = draw_bits4(jax.random.fold_in(arg_keys[8], 71), 0)
    w_in = normal_values(arg_keys[5], (3, 3, C, HID), (9 * C) ** -0.5, 0.375)
    w_mid = normal_values(arg_keys[6], (3, 3, HID, HID), (9 * HID) ** -0.5, 0.125)
    w_out = normal_values(arg_keys[7], (3, 3, C, HID), (9 * HID) ** -0.5, 0.125)
    return {"latent": latent, "bits1": bits1, "bits2": bits2, "bits3": bits3, "bits4": bits4, "w_in": w_in, "w_mid": w_mid, "w_out": w_out}


sharpness = 2.0
epsilon = 1e-6


def make_codes(group_bits):
    code_ids = jnp.arange(2 ** group_bits, dtype=jnp.int32)[:, None]
    bit_place = jnp.arange(group_bits, dtype=jnp.int32)[None, :]
    return ((code_ids // (2 ** (group_bits - 1 - bit_place))) % 2).astype(jnp.float32)


def bilinear(first_row, row_count, factor, grid_side, offset, columns):
    targets = first_row + jnp.arange(row_count, dtype=jnp.int32)
    numerator = 2 * targets + 1 - factor
    lower_idx = numerator // (2 * factor)
    fraction = (numerator - 2 * factor * lower_idx).astype(jnp.float32) / (2.0 * factor)
    lower_col = jnp.clip(lower_idx, 0, grid_side - 1) - offset
    upper_col = jnp.clip(lower_idx + 1, 0, grid_side - 1) - offset
    col_ids = jnp.arange(columns, dtype=jnp.int32)[None, :]
    low_hit = (col_ids == lower_col[:, None]).astype(jnp.float32)
    high_hit = (col_ids == upper_col[:, None]).astype(jnp.float32)
    return (1.0 - fraction)[:, None] * low_hit + fraction[:, None] * high_hit


def level_stats(logits, bit_table):
    probs = jax.nn.sigmoid(logits)
    soft_plus = jax.nn.softplus(logits)
    soft_minus = jax.nn.softplus(-logits)
    entropy = jnp.sum(probs * soft_minus + (1.0 - probs) * soft_plus)
    group_bits = bit_table.shape[1]
    shape = logits.shape
    grouped = (shape[0], shape[1], shape[2] // group_bits, group_bits, shape[3])
    log_one = (-soft_minus).reshape(grouped)
    log_zero = (-soft_plus).reshape(grouped)
    log_codes = jnp.einsum('jb,ntgbs->ntgjs', bit_table, log_one, precision=lax.Precision.HIGHEST)
    log_codes = log_codes + jnp.einsum('jb,ntgbs->ntgjs', 1.0 - bit_table, log_zero, precision=lax.Precision.HIGHEST)
    usage_sum = jnp.sum(jnp.exp(log_codes), axis=(0, 1, 4))
    return usage_sum, entropy


def conv_exact(extended, weights, row_count, out_first):
    padded = jnp.pad(extended, ((0, 0), (0, 0), (0, 0), (1, 1)))
    col_count = extended.shape[3]
    einsum_form = 'knrcw,koc->nrow' if out_first else 'knrcw,kco->nrow'
    total = None
    for row_shift in range(3):
        windows = jnp.stack([padded[:, row_shift:row_shift + row_count, :, col_shift:col_shift + col_count] for col_shift in range(3)])
        partial_sum = jnp.einsum(einsum_form, windows, weights[row_shift].astype(jnp.float32), precision=lax.Precision.HIGHEST)
        total = partial_sum if total is None else total + partial_sum
    return total


def to_half(values):
    return lax.optimization_barrier(values.astype(jnp.bfloat16)).astype(jnp.float32)


def pad_rows(values):
    return jnp.pad(values, ((0, 0), (1, 1), (0, 0), (0, 0)))


def refine_image(image, w_in, w_mid, w_out):
    row_count = image.shape[0]
    rounded = to_half(image)[None]
    first = to_half(jax.nn.gelu(conv_exact(pad_rows(rounded), w_in, row_count, False)))
    second = to_half(jax.nn.gelu(conv_exact(pad_rows(first), w_mid, row_count, False)))
    return conv_exact(pad_rows(second), w_out, row_count, True)[0]


def reference(latent, bits1, bits2, bits3, bits4, w_in, w_mid, w_out):
    images, height, channels, col_count = latent.shape
    bit_table = make_codes(GB)
    recon = jnp.zeros(latent.shape, jnp.float32)
    usage_list = []
    entropy_list = []
    for level_bits in (bits1, bits2, bits3, bits4):
        grid_side = level_bits.shape[3]
        factor = col_count // grid_side
        residual = latent - recon
        coarse = residual.reshape(images, grid_side, factor, channels, grid_side, factor).mean(axis=(2, 5))
        magnitude = jnp.sum(jnp.abs(coarse), axis=(1, 3)) / (grid_side * grid_side)
        quantized = level_bits.astype(jnp.float32) * magnitude[:, None, :, None]
        usage_sum, entropy = level_stats(sharpness * factor * coarse, bit_table)
        positions = images * grid_side * grid_side
        usage_list.append(usage_sum / positions)
        entropy_list.append(entropy / (positions * channels))
        if factor == 1:
            upsampled = quantized
        else:
            row_table = bilinear(0, height, factor, grid_side, 0, grid_side)
            col_table = bilinear(0, col_count, factor, grid_side, 0, grid_side)
            upsampled = jnp.einsum('is,nsct->nict', row_table, quantized, precision=lax.Precision.HIGHEST)
            upsampled = jnp.einsum('nict,jt->nicj', upsampled, col_table, precision=lax.Precision.HIGHEST)
        branch = lax.map(partial(refine_image, w_in=w_in, w_mid=w_mid, w_out=w_out), upsampled)
        recon = recon + upsampled + branch
    usage_mean = jnp.stack(usage_list)
    usage_entropy = -jnp.sum(usage_mean * jnp.log(usage_mean + epsilon), axis=-1)
    sample_entropy = jnp.stack(entropy_list)
    return recon, usage_entropy, sample_entropy
```

```python
import functools

import jax
import jax.numpy as jnp
from jax import lax
from jax.experimental import pallas as pl
from jax.experimental.pallas import tpu as pltpu
from jax.sharding import PartitionSpec as P

MESH = pl.DeviceIdType.MESH
F32 = jnp.float32
BF16 = jnp.bfloat16
FACTORS = (8, 4, 2, 1)
HALO = (1, 2, 2, 3)
SHARPNESS = 2.0
EPSILON = 1e-6
ROWS = 16
CH = 32
HID = 256
W = 128
PAIRS = ROWS // 2


def lanes(shape):
    return lax.broadcasted_iota(jnp.int32, shape, len(shape) - 1)


def subs(shape):
    return lax.broadcasted_iota(jnp.int32, shape, len(shape) - 2)


def side_masks(dtype):
    lane = lanes((1, W))
    low = jnp.where(lane == 0, 0.0, 1.0).astype(dtype)
    high = jnp.where(lane == W - 1, 0.0, 1.0).astype(dtype)
    return low, high


def from_left(x, low):
    return pltpu.roll(x, 1, 1) * low


def from_right(x, high):
    return pltpu.roll(x, W - 1, 1) * high


def gelu(x):
    inner = x * (0.7978845608028654 + (0.7978845608028654 * 0.044715) * (x * x))
    half = 0.5 * x
    return half + half * jnp.tanh(inner)


def block_mean(x, factor):
    lane = lanes(x.shape)
    step = 1
    while step < factor:
        below = pltpu.roll(x, step, 1)
        above = pltpu.roll(x, W - step, 1)
        x = x + jnp.where((lane & step) == 0, above, below)
        step *= 2
    return x * (1.0 / (factor * factor))


def column_table(side, factor):
    shape = (side, W)
    target = lanes(shape)
    row = subs(shape)
    shift = (2 * factor).bit_length() - 1
    numerator = 2 * target + 1 - factor
    lower = lax.shift_right_arithmetic(numerator, jnp.full(shape, shift, jnp.int32))
    fraction = (numerator - 2 * factor * lower).astype(F32) * (1.0 / (2.0 * factor))
    low_at = jnp.clip(lower, 0, side - 1)
    high_at = jnp.clip(lower + 1, 0, side - 1)
    table = jnp.where(row == low_at, 1.0 - fraction, 0.0) + jnp.where(
        row == high_at, fraction, 0.0
    )
    return table.astype(BF16)


def body(
    ny,
    nz,
    nr,
    lat,
    b1,
    b2,
    b3,
    b4,
    w_in,
    w_mid,
    w_out,
    recon,
    uent,
    sent,
    w1,
    w2,
    w3,
    xs,
    fs,
    gs,
    ub,
    cs,
    ps,
    qs,
    h1,
    h2,
    h3,
    h4,
    mags,
    tot,
    part_r,
    part_y,
    part_z,
    halo_ss,
    halo_rs,
    mag_ss,
    mag_rs,
    pr_ss,
    pr_rs,
    py_ss,
    py_rs,
    pz_ss,
    pz_rs,
):
    bits = (b1, b2, b3, b4)
    halos = (h1, h2, h3, h4)
    me = lax.axis_index("rows")
    dp = lax.axis_index("dp")
    my_y = dp // nz
    my_z = dp % nz
    is_first = me == 0
    is_last = me == nr - 1

    def row_peer(d):
        return lax.rem(me + d, nr)

    def y_peer(d):
        return lax.rem(my_y + d, ny)

    def z_peer(d):
        return lax.rem(my_z + d, nz)

    barrier = pltpu.get_barrier_semaphore()
    for d in range(1, nr):
        pl.semaphore_signal(barrier, inc=1, device_id={"rows": row_peer(d)}, device_id_type=MESH)
    for d in range(1, ny):
        pl.semaphore_signal(
            barrier, inc=1, device_id={"dp": y_peer(d) * nz + my_z}, device_id_type=MESH
        )
    for d in range(1, nz):
        pl.semaphore_signal(
            barrier, inc=1, device_id={"dp": my_y * nz + z_peer(d)}, device_id_type=MESH
        )

    def halo_copy(level, side):
        count = ROWS // FACTORS[level]
        keep = HALO[level]
        if side == 0:
            src = bits[level].at[0, pl.ds(count - keep, keep)]
            target = me + 1
        else:
            src = bits[level].at[0, pl.ds(0, keep)]
            target = me - 1
        return pltpu.make_async_remote_copy(
            src_ref=src,
            dst_ref=halos[level].at[side],
            send_sem=halo_ss.at[level, side],
            recv_sem=halo_rs.at[level, side],
            device_id={"rows": target},
            device_id_type=MESH,
        )

    def halo_send(level):
        @pl.when(jnp.logical_not(is_last))
        def _():
            halo_copy(level, 0).start()

        @pl.when(jnp.logical_not(is_first))
        def _():
            halo_copy(level, 1).start()

    def halo_wait(level):
        @pl.when(jnp.logical_not(is_first))
        def _():
            halo_copy(level, 0).wait_recv()

        @pl.when(jnp.logical_not(is_last))
        def _():
            halo_copy(level, 1).wait_recv()

    def halo_drain(level):
        @pl.when(jnp.logical_not(is_last))
        def _():
            halo_copy(level, 0).wait_send()

        @pl.when(jnp.logical_not(is_first))
        def _():
            halo_copy(level, 1).wait_send()

    def mag_copy(level, d, slot):
        return pltpu.make_async_remote_copy(
            src_ref=mags.at[level, slot],
            dst_ref=mags.at[level, slot],
            send_sem=mag_ss.at[level, d],
            recv_sem=mag_rs.at[level, slot],
            device_id={"rows": row_peer(d)},
            device_id_type=MESH,
        )

    def stage_copy(buf, ss, rs, d, slot, target):
        return pltpu.make_async_remote_copy(
            src_ref=buf.at[slot],
            dst_ref=buf.at[slot],
            send_sem=ss.at[d],
            recv_sem=rs.at[slot],
            device_id=target,
            device_id_type=MESH,
        )

    def r_copy(d, slot):
        return stage_copy(part_r, pr_ss, pr_rs, d, slot, {"rows": row_peer(d)})

    def y_copy(d, slot):
        return stage_copy(part_y, py_ss, py_rs, d, slot, {"dp": y_peer(d) * nz + my_z})

    def z_copy(d, slot):
        return stage_copy(part_z, pz_ss, pz_rs, d, slot, {"dp": my_y * nz + z_peer(d)})

    def residual_row(level, row):
        if level == 0:
            return lat[0, row]
        return lat[0, row] - recon[0, row]

    def coarse_stage(level):
        factor = FACTORS[level]
        count = ROWS // factor
        total = jnp.zeros((CH, W), F32)
        for i in range(count):
            acc = residual_row(level, i * factor)
            for j in range(1, factor):
                acc = acc + residual_row(level, i * factor + j)
            acc = block_mean(acc, factor)
            cs[i] = acc
            total = total + jnp.abs(acc)
        summed = jnp.sum(total, axis=1, keepdims=True)
        shape = (CH, W)
        row = jnp.sum(
            jnp.where(lanes(shape) == subs(shape), jnp.broadcast_to(summed, shape), 0.0),
            axis=0,
            keepdims=True,
        )
        mags[level, me] = row

    def mag_send(level):
        for d in range(1, nr):
            mag_copy(level, d, me).start()

    def mag_wait(level):
        for d in range(1, nr):
            mag_copy(level, d, row_peer(d)).wait_recv()
        factor = FACTORS[level]
        side = W // factor
        row = mags[level, 0]
        for j in range(1, nr):
            row = row + mags[level, j]
        shape = (CH, W)
        spread = jnp.where(lanes(shape) == subs(shape), jnp.broadcast_to(row, shape), 0.0)
        return jnp.sum(spread, axis=1, keepdims=True) * (1.0 / (factor * side * side))

    def stats_stage(level):
        factor = FACTORS[level]
        count = ROWS // factor
        entropy = jnp.zeros((8, W), F32)
        for i in range(count):
            logits = (SHARPNESS * factor) * cs[i]
            size = jnp.abs(logits)
            small = jnp.exp(-size)
            inverse = 1.0 / (1.0 + small)
            rest = small * inverse
            each = jnp.log1p(small) + size * rest
            entropy = entropy + (each[0:8] + each[8:16]) + (each[16:24] + each[24:32])
            positive = logits >= 0.0
            ps[i] = jnp.where(positive, inverse, rest)
            qs[i] = jnp.where(positive, rest, inverse)
        sums = [jnp.zeros((8, W), F32) for _ in range(16)]
        for i in range(count):
            one = [ps[i, pl.ds(k, 8, stride=4)] for k in range(4)]
            zero = [qs[i, pl.ds(k, 8, stride=4)] for k in range(4)]
            front = [x * y for x in (zero[0], one[0]) for y in (zero[1], one[1])]
            back = [x * y for x in (zero[2], one[2]) for y in (zero[3], one[3])]
            for j in range(16):
                sums[j] = sums[j] + front[j // 4] * back[j % 4]
        lane = lanes((8, W))
        tile = jnp.zeros((8, W), F32) if level == 0 else tot[...]
        for j in range(16):
            tile = tile + jnp.where(
                lane == level * 16 + j, jnp.sum(sums[j], axis=1, keepdims=True), 0.0
            )
        tile = tile + jnp.where(lane == 64 + level, jnp.sum(entropy, axis=1, keepdims=True), 0.0)
        tot[...] = tile

    def spread_stage(level):
        factor = FACTORS[level]
        count = ROWS // factor
        keep = HALO[level]
        side = W // factor
        ref = bits[level]
        top = halos[level][0]
        bottom = halos[level][1]
        own_top = jnp.broadcast_to(ref[0, 0][None], (keep, CH, side))
        own_bottom = jnp.broadcast_to(ref[0, count - 1][None], (keep, CH, side))
        top = jnp.where(is_first, own_top, top)
        bottom = jnp.where(is_last, own_bottom, bottom)
        if factor == 1:
            for u in range(3):
                ub[u] = top[u].astype(F32)
                ub[ROWS + 3 + u] = bottom[u].astype(F32)
            for u in range(ROWS):
                ub[u + 3] = ref[0, u].astype(F32)
            return
        stack = jnp.concatenate([top, ref[0], bottom], axis=0).astype(F32).astype(BF16)
        stack = stack.reshape((count + 2 * keep) * CH, side)
        wide = jnp.dot(stack, column_table(side, factor), preferred_element_type=F32)
        wide = wide.reshape(count + 2 * keep, CH, W)
        for u in range(ROWS + 6):
            numerator = 2 * (u - 3) + 1 - factor
            lower = numerator // (2 * factor)
            fraction = (numerator - 2 * factor * lower) / (2.0 * factor)
            at = lower + keep
            ub[u] = (1.0 - fraction) * wide[at] + fraction * wide[at + 1]

    def scale_stage(level, magnitude):
        low, high = side_masks(BF16)
        wide = jnp.broadcast_to(magnitude, (CH, W))
        top = jnp.where(is_first, 0.0, 1.0)
        bottom = jnp.where(is_last, 0.0, 1.0)
        for u in range(ROWS + 6):
            up = ub[u] * wide
            if u < 3:
                up = up * top
            elif u >= ROWS + 3:
                up = up * bottom
            elif level == 0:
                recon[0, u - 3] = up
            else:
                recon[0, u - 3] = recon[0, u - 3] + up
            half = up.astype(BF16)
            xs[u, 0:CH] = from_left(half, low)
            xs[u, CH : 2 * CH] = half
            xs[u, 2 * CH : 3 * CH] = from_right(half, high)

    def window(ref, row):
        a = ref[row : row + 3]
        b = ref[row + 1 : row + 4]
        depth = 3 * a.shape[1]
        return jnp.concatenate([a.reshape(depth, W), b.reshape(depth, W)], axis=1)

    def first_pair(p):
        low, high = side_masks(BF16)
        z = gelu(jnp.dot(w1[...], window(xs, 2 * p), preferred_element_type=F32))
        if p == 0:
            z = z * jnp.where(is_first, 0.0, 1.0)
        if p == PAIRS + 1:
            z = z * jnp.where(is_last, 0.0, 1.0)
        z = z.astype(BF16)
        for h in range(2):
            x = z[:, h * W : (h + 1) * W]
            fs[2 * p + h, 0:HID] = from_left(x, low)
            fs[2 * p + h, HID : 2 * HID] = x
            fs[2 * p + h, 2 * HID : 3 * HID] = from_right(x, high)

    def second_pair(p):
        z = gelu(jnp.dot(w2[...], window(fs, 2 * p), preferred_element_type=F32))
        for h in range(2):
            x = z[:, h * W : (h + 1) * W]
            if p == 0 and h == 0:
                x = x * jnp.where(is_first, 0.0, 1.0)
            if p == PAIRS and h == 1:
                x = x * jnp.where(is_last, 0.0, 1.0)
            gs[2 * p + h] = x.astype(BF16)

    def third_pair(p):
        low, high = side_masks(F32)
        z = jnp.dot(w3[...], window(gs, 2 * p), preferred_element_type=F32)
        for h in range(2):
            x = z[:, h * W : (h + 1) * W]
            recon[0, 2 * p + h] = recon[0, 2 * p + h] + (
                x[CH : 2 * CH] + from_left(x[0:CH], low) + from_right(x[2 * CH : 3 * CH], high)
            )

    flat_in = w_in[...].reshape(9 * CH, HID)
    w1[...] = flat_in.T
    for tap in range(9):
        w2[:, tap * HID : (tap + 1) * HID] = w_mid[tap // 3, tap % 3].T
    for dr in range(3):
        for dc in range(3):
            w3[dc * CH : (dc + 1) * CH, dr * HID : (dr + 1) * HID] = w_out[dr, dc]

    coarse_stage(0)
    pl.semaphore_wait(barrier, (nr - 1) + (ny - 1) + (nz - 1))
    mag_send(0)
    halo_send(0)
    for level in range(1, 4):
        halo_send(level)

    def one_level(level, _):
        for k in range(4):

            @pl.when(level == k)
            def _(k=k):
                if k > 0:
                    coarse_stage(k)
                    mag_send(k)
                stats_stage(k)
                halo_wait(k)
                spread_stage(k)
                if k == 3:
                    part_r[me] = tot[...]
                    for d in range(1, nr):
                        r_copy(d, me).start()
                scale_stage(k, mag_wait(k))

        for p in range(PAIRS + 4):
            if p < PAIRS + 2:
                first_pair(p)
            if 2 <= p < PAIRS + 3:
                second_pair(p - 2)
            if p >= 4:
                third_pair(p - 4)
            if p == 4:

                @pl.when(level == 3)
                def _():
                    for d in range(1, nr):
                        r_copy(d, row_peer(d)).wait_recv()
                    tile = part_r[0]
                    for j in range(1, nr):
                        tile = tile + part_r[j]
                    part_y[my_y] = tile
                    for d in range(1, ny):
                        y_copy(d, my_y).start()

            if p == 7:

                @pl.when(level == 3)
                def _():
                    for d in range(1, ny):
                        y_copy(d, y_peer(d)).wait_recv()
                    tile = part_y[0]
                    for j in range(1, ny):
                        tile = tile + part_y[j]
                    part_z[my_z] = tile
                    for d in range(1, nz):
                        z_copy(d, my_z).start()

        return 0

    lax.fori_loop(0, 4, one_level, 0)

    for d in range(1, nz):
        z_copy(d, z_peer(d)).wait_recv()
    tile = part_z[0]
    for j in range(1, nz):
        tile = tile + part_z[j]
    lane = lanes((8, W))
    images = ny * nz
    group = lane // 16
    scale = jnp.zeros((8, W), F32)
    for level in range(4):
        side = W // FACTORS[level]
        scale = jnp.where(
            group == level, 1.0 / (images * side * side * FACTORS[level]), scale
        )
    usage = tile * scale
    terms = -(usage * jnp.log(usage + EPSILON))
    square = (8, W)
    for level in range(4):
        mine = jnp.sum(jnp.where(group == level, terms, 0.0), axis=1, keepdims=True)
        row = jnp.sum(
            jnp.where(lanes(square) == subs(square), jnp.broadcast_to(mine, square), 0.0),
            axis=0,
            keepdims=True,
        )
        uent[level : level + 1, :] = row[:, 0:8]
    entropies = jnp.sum(tile, axis=0, keepdims=True)
    shifted = pltpu.roll(entropies, W - 64, 1)
    lane1 = lanes((1, W))
    scale1 = jnp.zeros((1, W), F32)
    for level in range(4):
        side = W // FACTORS[level]
        scale1 = jnp.where(
            lane1 == level, 1.0 / (images * side * side * FACTORS[level] * CH), scale1
        )
    sent[...] = (shifted * scale1)[:, 0:4]

    for level in range(4):
        halo_drain(level)
        for d in range(1, nr):
            mag_copy(level, d, me).wait_send()
    for d in range(1, nr):
        r_copy(d, me).wait_send()
    for d in range(1, ny):
        y_copy(d, my_y).wait_send()
    for d in range(1, nz):
        z_copy(d, my_z).wait_send()


def solution(mesh):
    nd = mesh.shape["dp"]
    nr = mesh.shape["rows"]
    ny = 4 if nd % 4 == 0 and nd >= 16 else 1
    nz = nd // ny

    vmem = pl.BlockSpec(memory_space=pltpu.VMEM)
    dma = pltpu.SemaphoreType.DMA

    def on_device(*args):
        recon, uent, sent = pl.pallas_call(
            functools.partial(body, ny, nz, nr),
            out_shape=(
                jax.ShapeDtypeStruct((1, ROWS, CH, W), F32),
                jax.ShapeDtypeStruct((4, 8), F32),
                jax.ShapeDtypeStruct((1, 4), F32),
            ),
            in_specs=[vmem] * 8,
            out_specs=(vmem, vmem, vmem),
            scratch_shapes=[
                pltpu.VMEM((HID, 9 * CH), BF16),
                pltpu.VMEM((HID, 9 * HID), BF16),
                pltpu.VMEM((3 * CH, 3 * HID), BF16),
                pltpu.VMEM((ROWS + 6, 3 * CH, W), BF16),
                pltpu.VMEM((ROWS + 4, 3 * HID, W), BF16),
                pltpu.VMEM((ROWS + 2, HID, W), BF16),
                pltpu.VMEM((ROWS + 6, CH, W), F32),
                pltpu.VMEM((ROWS, CH, W), F32),
                pltpu.VMEM((ROWS, CH, W), F32),
                pltpu.VMEM((ROWS, CH, W), F32),
                pltpu.VMEM((2, HALO[0], CH, 16), jnp.int32),
                pltpu.VMEM((2, HALO[1], CH, 32), jnp.int32),
                pltpu.VMEM((2, HALO[2], CH, 64), jnp.int32),
                pltpu.VMEM((2, HALO[3], CH, 128), jnp.int32),
                pltpu.VMEM((4, nr, 1, W), F32),
                pltpu.VMEM((8, W), F32),
                pltpu.VMEM((nr, 8, W), F32),
                pltpu.VMEM((ny, 8, W), F32),
                pltpu.VMEM((nz, 8, W), F32),
                dma((4, 2)),
                dma((4, 2)),
                dma((4, nr)),
                dma((4, nr)),
                dma((nr,)),
                dma((nr,)),
                dma((ny,)),
                dma((ny,)),
                dma((nz,)),
                dma((nz,)),
            ],
            compiler_params=pltpu.CompilerParams(
                collective_id=0, has_side_effects=True, vmem_limit_bytes=60 * 1024 * 1024
            ),
        )(*args)
        return recon, uent, sent.reshape(4)

    split = P("dp", "rows", None, None)
    return jax.shard_map(
        on_device,
        mesh=mesh,
        in_specs=(split,) * 5 + (P(),) * 3,
        out_specs=(split, P(), P()),
        check_vma=False,
    )
```

```python
import functools

import jax
import jax.numpy as jnp
from jax import lax
from jax.experimental import pallas as pl
from jax.experimental.pallas import tpu as pltpu
from jax.sharding import PartitionSpec as P

MESH = pl.DeviceIdType.MESH
F32 = jnp.float32
BF16 = jnp.bfloat16
FACTORS = (8, 4, 2, 1)
HALO = (1, 2, 2, 3)
SHARPNESS = 2.0
EPSILON = 1e-6
VMEM_LIMIT = 66000000
ROWS = 16
CH = 32
HID = 256
W = 128
PAIRS = ROWS // 2
SPLIT = (0, PAIRS)


def lanes(shape):
    return lax.broadcasted_iota(jnp.int32, shape, len(shape) - 1)


def subs(shape):
    return lax.broadcasted_iota(jnp.int32, shape, len(shape) - 2)


def side_masks(dtype):
    lane = lanes((1, W))
    low = jnp.where(lane == 0, 0.0, 1.0).astype(dtype)
    high = jnp.where(lane == W - 1, 0.0, 1.0).astype(dtype)
    return low, high


def from_left(x, low):
    return pltpu.roll(x, 1, 1) * low


def from_right(x, high):
    return pltpu.roll(x, W - 1, 1) * high


def gelu(x):
    inner = x * (0.7978845608028654 + (0.7978845608028654 * 0.044715) * (x * x))
    half = 0.5 * x
    return half + half * jnp.tanh(inner)


def block_mean(x, factor):
    lane = lanes(x.shape)
    step = 1
    while step < factor:
        below = pltpu.roll(x, step, 1)
        above = pltpu.roll(x, W - step, 1)
        x = x + jnp.where((lane & step) == 0, above, below)
        step *= 2
    return x * (1.0 / (factor * factor))


def column_table(side, factor):
    shape = (side, W)
    target = lanes(shape)
    row = subs(shape)
    shift = (2 * factor).bit_length() - 1
    numerator = 2 * target + 1 - factor
    lower = lax.shift_right_arithmetic(numerator, jnp.full(shape, shift, jnp.int32))
    fraction = (numerator - 2 * factor * lower).astype(F32) * (1.0 / (2.0 * factor))
    low_at = jnp.clip(lower, 0, side - 1)
    high_at = jnp.clip(lower + 1, 0, side - 1)
    table = jnp.where(row == low_at, 1.0 - fraction, 0.0) + jnp.where(
        row == high_at, fraction, 0.0
    )
    return table.astype(BF16)


def body(
    ny,
    nz,
    nr,
    lat_in,
    b1_in,
    b2_in,
    b3_in,
    b4_in,
    w_in_in,
    w_mid_in,
    w_out_in,
    recon,
    final,
    lat,
    b1,
    b2,
    b3,
    b4,
    w_in,
    w_mid,
    w_out,
    w1,
    w2,
    w3,
    xs,
    fs,
    gs,
    ub,
    cs,
    ps,
    qs,
    h1,
    h2,
    h3,
    h4,
    mags,
    mg,
    st,
    part_r,
    part_d,
    in_sem,
    halo_ss,
    halo_rs,
    mag_ss,
    mag_rs,
    pr_ss,
    pr_rs,
    pd_ss,
    pd_rs,
    near,
):
    bits = (b1, b2, b3, b4)
    halos = (h1, h2, h3, h4)
    me = lax.axis_index("rows")
    dp = lax.axis_index("dp")
    my_y = dp // nz
    my_z = dp % nz
    is_first = me == 0
    is_last = me == nr - 1

    def row_peer(d):
        return lax.rem(me + d, nr)

    def dp_peer(d):
        return lax.rem(my_y + d // nz, ny) * nz + lax.rem(my_z + d % nz, nz)

    steps = [] if nz == 1 else [1, nz - 1]
    steps = steps + ([] if ny == 1 else [nz, (ny - 1) * nz])

    barrier = pltpu.get_barrier_semaphore()
    for d in range(1, nr):
        pl.semaphore_signal(barrier, inc=1, device_id={"rows": row_peer(d)}, device_id_type=MESH)
    for d in steps:
        pl.semaphore_signal(barrier, inc=1, device_id={"dp": dp_peer(d)}, device_id_type=MESH)

    def near_send():
        for n, d in enumerate(steps):
            pl.semaphore_signal(
                near.at[n], inc=1, device_id={"dp": dp_peer(d)}, device_id_type=MESH
            )

    def near_wait():
        for n in range(len(steps)):
            pl.semaphore_wait(near.at[n], 1)

    hbm = (lat_in, b1_in, w_in_in, w_out_in, w_mid_in, b2_in, b3_in, b4_in)
    local = (lat, b1, w_in, w_out, w_mid, b2, b3, b4)

    def fetch(n):
        return pltpu.make_async_copy(hbm[n], local[n], in_sem.at[n])

    for n in range(8):
        fetch(n).start()

    def halo_copy(level, side):
        count = ROWS // FACTORS[level]
        keep = HALO[level]
        if side == 0:
            src = bits[level].at[0, pl.ds(count - keep, keep)]
            target = me + 1
        else:
            src = bits[level].at[0, pl.ds(0, keep)]
            target = me - 1
        return pltpu.make_async_remote_copy(
            src_ref=src,
            dst_ref=halos[level].at[side],
            send_sem=halo_ss.at[level, side],
            recv_sem=halo_rs.at[level, side],
            device_id={"rows": target},
            device_id_type=MESH,
        )

    def halo_send(level):
        @pl.when(jnp.logical_not(is_last))
        def _():
            halo_copy(level, 0).start()

        @pl.when(jnp.logical_not(is_first))
        def _():
            halo_copy(level, 1).start()

    def halo_wait(level):
        @pl.when(jnp.logical_not(is_first))
        def _():
            halo_copy(level, 0).wait_recv()

        @pl.when(jnp.logical_not(is_last))
        def _():
            halo_copy(level, 1).wait_recv()

    def halo_drain(level):
        @pl.when(jnp.logical_not(is_last))
        def _():
            halo_copy(level, 0).wait_send()

        @pl.when(jnp.logical_not(is_first))
        def _():
            halo_copy(level, 1).wait_send()

    def mag_copy(level, d, slot):
        return pltpu.make_async_remote_copy(
            src_ref=mags.at[level, slot],
            dst_ref=mags.at[level, slot],
            send_sem=mag_ss.at[level, d],
            recv_sem=mag_rs.at[level, slot],
            device_id={"rows": row_peer(d)},
            device_id_type=MESH,
        )

    def stage_copy(buf, ss, rs, d, slot, target):
        return pltpu.make_async_remote_copy(
            src_ref=buf.at[slot],
            dst_ref=buf.at[slot],
            send_sem=ss.at[d],
            recv_sem=rs.at[slot],
            device_id=target,
            device_id_type=MESH,
        )

    def r_copy(d, slot):
        return stage_copy(part_r, pr_ss, pr_rs, d, slot, {"rows": row_peer(d)})

    def d_copy(d, slot):
        return stage_copy(part_d, pd_ss, pd_rs, d, slot, {"dp": dp_peer(d)})

    def residual_row(level, row):
        if level == 0:
            return lat[0, row]
        return lat[0, row] - recon[0, row]

    def coarse_stage(level):
        factor = FACTORS[level]
        count = ROWS // factor
        total = jnp.zeros((CH, W), F32)
        for i in range(count):
            acc = residual_row(level, i * factor)
            for j in range(1, factor):
                acc = acc + residual_row(level, i * factor + j)
            acc = block_mean(acc, factor)
            cs[i] = acc
            total = total + jnp.abs(acc)
        summed = jnp.sum(total, axis=1, keepdims=True)
        shape = (CH, W)
        row = jnp.sum(
            jnp.where(lanes(shape) == subs(shape), jnp.broadcast_to(summed, shape), 0.0),
            axis=0,
            keepdims=True,
        )
        mags[level, me] = row

    def mag_send(level):
        for d in range(1, nr):
            mag_copy(level, d, me).start()

    def mag_wait(level):
        for d in range(1, nr):
            mag_copy(level, d, row_peer(d)).wait_recv()
        factor = FACTORS[level]
        side = W // factor
        row = mags[level, 0]
        for j in range(1, nr):
            row = row + mags[level, j]
        shape = (CH, W)
        spread = jnp.where(lanes(shape) == subs(shape), jnp.broadcast_to(row, shape), 0.0)
        return jnp.sum(spread, axis=1, keepdims=True) * (1.0 / (factor * side * side))

    def stats_stage(level):
        factor = FACTORS[level]
        count = ROWS // factor
        entropy = jnp.zeros((8, W), F32)
        for i in range(count):
            logits = (SHARPNESS * factor) * cs[i]
            size = jnp.abs(logits)
            small = jnp.exp(-size)
            inverse = 1.0 / (1.0 + small)
            rest = small * inverse
            each = jnp.log1p(small) + size * rest
            entropy = entropy + (each[0:8] + each[8:16]) + (each[16:24] + each[24:32])
            positive = logits >= 0.0
            ps[i] = jnp.where(positive, inverse, rest)
            qs[i] = jnp.where(positive, rest, inverse)
        sums = [jnp.zeros((8, W), F32) for _ in range(16)]
        for i in range(count):
            one = [ps[i, pl.ds(k, 8, stride=4)] for k in range(4)]
            zero = [qs[i, pl.ds(k, 8, stride=4)] for k in range(4)]
            front = [x * y for x in (zero[0], one[0]) for y in (zero[1], one[1])]
            back = [x * y for x in (zero[2], one[2]) for y in (zero[3], one[3])]
            for j in range(16):
                sums[j] = sums[j] + front[j // 4] * back[j % 4]
        lane = lanes((8, W))
        place = lane - 16 * subs((8, W))
        tile = jnp.zeros((8, W), F32)
        for j in range(16):
            tile = tile + jnp.where(place == j, jnp.sum(sums[j], axis=1, keepdims=True), 0.0)
        st[level] = jnp.sum(tile, axis=0, keepdims=True)
        flat = jnp.sum(
            jnp.where(lane == level, jnp.sum(entropy, axis=1, keepdims=True), 0.0),
            axis=0,
            keepdims=True,
        )
        st[4] = flat if level == 0 else st[4] + flat

    def spread_stage(level):
        factor = FACTORS[level]
        count = ROWS // factor
        keep = HALO[level]
        side = W // factor
        ref = bits[level]
        top = halos[level][0]
        bottom = halos[level][1]
        plane = (side, CH) if level == 0 else (CH, side)
        own_top = jnp.broadcast_to(ref[0, 0][None], (keep, *plane))
        own_bottom = jnp.broadcast_to(ref[0, count - 1][None], (keep, *plane))
        top = jnp.where(is_first, own_top, top)
        bottom = jnp.where(is_last, own_bottom, bottom)
        if factor == 1:
            for u in range(3):
                ub[u] = top[u].astype(F32)
                ub[ROWS + 3 + u] = bottom[u].astype(F32)
            for u in range(ROWS):
                ub[u + 3] = ref[0, u].astype(F32)
            return
        stack = jnp.concatenate([top, ref[0], bottom], axis=0).astype(F32).astype(BF16)
        table = column_table(side, factor)
        if level == 0:
            wide = [
                lax.dot_general(
                    stack[n], table, (((0,), (0,)), ((), ())), preferred_element_type=F32
                )
                for n in range(count + 2 * keep)
            ]
        else:
            stack = stack.reshape((count + 2 * keep) * CH, side)
            wide = jnp.dot(stack, table, preferred_element_type=F32)
            wide = wide.reshape(count + 2 * keep, CH, W)
        for u in range(ROWS + 6):
            numerator = 2 * (u - 3) + 1 - factor
            lower = numerator // (2 * factor)
            fraction = (numerator - 2 * factor * lower) / (2.0 * factor)
            at = lower + keep
            ub[u] = (1.0 - fraction) * wide[at] + fraction * wide[at + 1]

    def scale_row(u):
        low, high = side_masks(BF16)
        up = ub[u] * mg[...]
        if u < 3:
            up = up * jnp.where(is_first, 0.0, 1.0)
        elif u >= ROWS + 3:
            up = up * jnp.where(is_last, 0.0, 1.0)
        else:
            recon[0, u - 3] = recon[0, u - 3] + up
        half = up.astype(BF16)
        xs[u, 0:CH] = from_left(half, low)
        xs[u, CH : 2 * CH] = half
        xs[u, 2 * CH : 3 * CH] = from_right(half, high)

    def window(ref, row):
        a = ref[row : row + 3]
        b = ref[row + 1 : row + 4]
        depth = 3 * a.shape[1]
        return jnp.concatenate([a.reshape(depth, W), b.reshape(depth, W)], axis=1)

    def first_pair(p):
        low, high = side_masks(BF16)
        z = gelu(jnp.dot(w1[...], window(xs, 2 * p), preferred_element_type=F32))
        if p == 0:
            z = z * jnp.where(is_first, 0.0, 1.0)
        if p == PAIRS + 1:
            z = z * jnp.where(is_last, 0.0, 1.0)
        z = z.astype(BF16)
        for h in range(2):
            x = z[:, h * W : (h + 1) * W]
            fs[2 * p + h, 0:HID] = from_left(x, low)
            fs[2 * p + h, HID : 2 * HID] = x
            fs[2 * p + h, 2 * HID : 3 * HID] = from_right(x, high)

    def second_pair(p):
        cuts = 2 if p in SPLIT else 1
        size = HID // cuts
        for n in range(cuts):
            at = n * size
            z = gelu(
                jnp.dot(w2[at : at + size, :], window(fs, 2 * p), preferred_element_type=F32)
            )
            for h in range(2):
                x = z[:, h * W : (h + 1) * W]
                if p == 0 and h == 0:
                    x = x * jnp.where(is_first, 0.0, 1.0)
                if p == PAIRS and h == 1:
                    x = x * jnp.where(is_last, 0.0, 1.0)
                gs[2 * p + h, at : at + size] = x.astype(BF16)

    def third_pair(p):
        low, high = side_masks(F32)
        z = jnp.dot(w3[...], window(gs, 2 * p), preferred_element_type=F32)
        for h in range(2):
            x = z[:, h * W : (h + 1) * W]
            recon[0, 2 * p + h] = recon[0, 2 * p + h] + (
                x[CH : 2 * CH] + from_left(x[0:CH], low) + from_right(x[2 * CH : 3 * CH], high)
            )

    fetch(0).wait()
    coarse_stage(0)
    pl.semaphore_wait(barrier, nr - 1 + len(steps))
    mag_send(0)
    near_send()
    fetch(1).wait()
    halo_send(0)
    for n in (5, 6, 7):
        fetch(n).wait()
    for level in range(1, 4):
        halo_send(level)

    for n in (2, 3, 4):
        fetch(n).wait()
    w1[...] = w_in[...].reshape(9 * CH, HID).T
    for dr in range(3):
        for dc in range(3):
            w3[dc * CH : (dc + 1) * CH, dr * HID : (dr + 1) * HID] = w_out[dr, dc]
    for tap in range(9):
        w2[:, tap * HID : (tap + 1) * HID] = w_mid[tap // 3, tap % 3].T
    recon[...] = jnp.zeros_like(recon)

    def one_level(level, _):
        for k in range(4):

            @pl.when(level == k)
            def _(k=k):
                if k > 0:
                    coarse_stage(k)
                    mag_send(k)
                stats_stage(k)
                if k == 3:
                    part_r[me] = st[...]
                    for d in range(1, nr):
                        r_copy(d, me).start()
                halo_wait(k)
                spread_stage(k)
                near_wait()
                if k < 3:
                    near_send()
                mg[...] = jnp.broadcast_to(mag_wait(k), (CH, W))
                if k < 3:
                    near_wait()
                    near_send()
                else:
                    for d in range(1, nr):
                        r_copy(d, row_peer(d)).wait_recv()
                    total = part_r[0]
                    for j in range(1, nr):
                        total = total + part_r[j]
                    part_d[dp] = total
                    for d in range(1, ny * nz):
                        d_copy(d, dp).start()

        for u in range(ROWS + 6):
            scale_row(u)
        for p in range(PAIRS + 4):
            if p < PAIRS + 2:
                first_pair(p)
            if 2 <= p < PAIRS + 3:
                second_pair(p - 2)
            if p >= 4:
                third_pair(p - 4)
        return 0

    lax.fori_loop(0, 4, one_level, 0)

    for d in range(1, ny * nz):
        d_copy(d, dp_peer(d)).wait_recv()
    total = part_d[0]
    for j in range(1, ny * nz):
        total = total + part_d[j]
    final[...] = total

    for level in range(4):
        halo_drain(level)
        for d in range(1, nr):
            mag_copy(level, d, me).wait_send()
    for d in range(1, nr):
        r_copy(d, me).wait_send()
    for d in range(1, ny * nz):
        d_copy(d, dp).wait_send()


def finish(images, recon_in, sums, recon, uent, sent, sem):
    copy = pltpu.make_async_copy(recon_in, recon, sem)
    copy.start()
    for level in range(4):
        side = W // FACTORS[level]
        usage = sums[level] * (1.0 / (images * side * side * FACTORS[level]))
        terms = -(usage * jnp.log(usage + EPSILON))
        shape = (W, 8)
        group = subs(shape) // 16
        pick = jnp.where(group == lanes(shape), 1.0, 0.0)
        uent[level : level + 1, :] = jnp.dot(
            terms, pick, precision=lax.Precision.HIGHEST, preferred_element_type=F32
        )
    lane = lanes((1, W))
    scale = jnp.zeros((1, W), F32)
    for level in range(4):
        side = W // FACTORS[level]
        scale = jnp.where(
            lane == level, 1.0 / (images * side * side * FACTORS[level] * CH), scale
        )
    sent[...] = (sums[4] * scale)[:, 0:4]
    copy.wait()


def solution(mesh):
    nd = mesh.shape["dp"]
    nr = mesh.shape["rows"]
    ny = 4 if nd % 4 == 0 and nd >= 16 else 1
    nz = nd // ny

    vmem = pl.BlockSpec(memory_space=pltpu.VMEM)
    dma = pltpu.SemaphoreType.DMA

    def on_device(lat, b1, *rest):
        anywhere = pl.BlockSpec(memory_space=pl.ANY)
        recon, sums = pl.pallas_call(
            functools.partial(body, ny, nz, nr),
            out_shape=(
                jax.ShapeDtypeStruct((1, ROWS, CH, W), F32),
                jax.ShapeDtypeStruct((5, 1, W), F32),
            ),
            in_specs=[pl.BlockSpec(memory_space=pltpu.HBM)] * 8,
            out_specs=(vmem, vmem),
            scratch_shapes=[
                pltpu.VMEM((1, ROWS, CH, W), F32),
                pltpu.VMEM((1, 2, 16, CH), jnp.int32),
                pltpu.VMEM((1, 4, CH, 32), jnp.int32),
                pltpu.VMEM((1, 8, CH, 64), jnp.int32),
                pltpu.VMEM((1, ROWS, CH, W), jnp.int32),
                pltpu.VMEM((3, 3, CH, HID), BF16),
                pltpu.VMEM((3, 3, HID, HID), BF16),
                pltpu.VMEM((3, 3, CH, HID), BF16),
                pltpu.VMEM((HID, 9 * CH), BF16),
                pltpu.VMEM((HID, 9 * HID), BF16),
                pltpu.VMEM((3 * CH, 3 * HID), BF16),
                pltpu.VMEM((ROWS + 6, 3 * CH, W), BF16),
                pltpu.VMEM((ROWS + 4, 3 * HID, W), BF16),
                pltpu.VMEM((ROWS + 2, HID, W), BF16),
                pltpu.VMEM((ROWS + 6, CH, W), F32),
                pltpu.VMEM((ROWS, CH, W), F32),
                pltpu.VMEM((ROWS, CH, W), F32),
                pltpu.VMEM((ROWS, CH, W), F32),
                pltpu.VMEM((2, HALO[0], 16, CH), jnp.int32),
                pltpu.VMEM((2, HALO[1], CH, 32), jnp.int32),
                pltpu.VMEM((2, HALO[2], CH, 64), jnp.int32),
                pltpu.VMEM((2, HALO[3], CH, 128), jnp.int32),
                pltpu.VMEM((4, nr, 1, W), F32),
                pltpu.VMEM((CH, W), F32),
                pltpu.VMEM((5, 1, W), F32),
                pltpu.VMEM((nr, 5, 1, W), F32),
                pltpu.VMEM((nd, 5, 1, W), F32),
                dma((8,)),
                dma((4, 2)),
                dma((4, 2)),
                dma((4, nr)),
                dma((4, nr)),
                dma((nr,)),
                dma((nr,)),
                dma((nd,)),
                dma((nd,)),
                pltpu.SemaphoreType.REGULAR((4,)),
            ],
            compiler_params=pltpu.CompilerParams(
                collective_id=0, has_side_effects=True, vmem_limit_bytes=VMEM_LIMIT
            ),
        )(lat, jnp.swapaxes(b1, 2, 3), *rest)
        recon, uent, sent = pl.pallas_call(
            functools.partial(finish, nd),
            out_shape=(
                jax.ShapeDtypeStruct((1, ROWS, CH, W), F32),
                jax.ShapeDtypeStruct((4, 8), F32),
                jax.ShapeDtypeStruct((1, 4), F32),
            ),
            in_specs=[anywhere, vmem],
            out_specs=(anywhere, vmem, vmem),
            scratch_shapes=[dma],
            compiler_params=pltpu.CompilerParams(vmem_limit_bytes=1024 * 1024),
        )(recon, sums)
        return recon, uent, sent.reshape(4)

    split = P("dp", "rows", None, None)
    return jax.shard_map(
        on_device,
        mesh=mesh,
        in_specs=(split,) * 5 + (P(),) * 3,
        out_specs=(split, P(), P()),
        check_vma=False,
    )
```

```python
import functools

import jax
import jax.numpy as jnp
from jax import lax
from jax.experimental import pallas as pl
from jax.experimental.pallas import tpu as pltpu
from jax.sharding import PartitionSpec as P

MESH = pl.DeviceIdType.MESH
F32 = jnp.float32
BF16 = jnp.bfloat16
FACTORS = (8, 4, 2, 1)
HALO = (1, 2, 2, 3)
SHARPNESS = 2.0
EPSILON = 1e-6
VMEM_LIMIT = 56545000
PARTS = 2
ROWS = 16
CH = 32
HID = 256
W = 128
PAIRS = ROWS // 2
CUTS = 2
SPLIT = tuple(range(PAIRS + 1))


def lanes(shape):
    return lax.broadcasted_iota(jnp.int32, shape, len(shape) - 1)


def subs(shape):
    return lax.broadcasted_iota(jnp.int32, shape, len(shape) - 2)


def side_masks(dtype):
    lane = lanes((1, W))
    low = jnp.where(lane == 0, 0.0, 1.0).astype(dtype)
    high = jnp.where(lane == W - 1, 0.0, 1.0).astype(dtype)
    return low, high


def from_left(x, low):
    return pltpu.roll(x, 1, 1) * low


def from_right(x, high):
    return pltpu.roll(x, W - 1, 1) * high


def twice_gelu(x):
    inner = x * (0.7978845608028654 + (0.7978845608028654 * 0.044715) * (x * x))
    return x + x * jnp.tanh(inner)


def block_mean(x, factor):
    lane = lanes(x.shape)
    step = 1
    while step < factor:
        below = pltpu.roll(x, step, 1)
        above = pltpu.roll(x, W - step, 1)
        x = x + jnp.where((lane & step) == 0, above, below)
        step *= 2
    return x * (1.0 / (factor * factor))


def column_table(side, factor):
    shape = (side, W)
    target = lanes(shape)
    row = subs(shape)
    shift = (2 * factor).bit_length() - 1
    numerator = 2 * target + 1 - factor
    lower = lax.shift_right_arithmetic(numerator, jnp.full(shape, shift, jnp.int32))
    fraction = (numerator - 2 * factor * lower).astype(F32) * (1.0 / (2.0 * factor))
    low_at = jnp.clip(lower, 0, side - 1)
    high_at = jnp.clip(lower + 1, 0, side - 1)
    table = jnp.where(row == low_at, 1.0 - fraction, 0.0) + jnp.where(
        row == high_at, fraction, 0.0
    )
    return table.astype(BF16)


def body(
    ny,
    nz,
    nr,
    lat_in,
    b1_in,
    b2_in,
    b3_in,
    b4_in,
    w_in_in,
    w_mid_in,
    w_out_in,
    recon_out,
    final,
    recon,
    lat,
    b1,
    b2,
    b3,
    b4,
    w_in,
    w_mid,
    w_out,
    w1,
    w2,
    w3,
    xs,
    fs,
    gs,
    ub,
    cs,
    ps,
    qs,
    h1,
    h2,
    h3,
    h4,
    mags,
    mg,
    st,
    part_r,
    part_d,
    in_sem,
    out_sem,
    halo_ss,
    halo_rs,
    mag_ss,
    mag_rs,
    pr_ss,
    pr_rs,
    pd_ss,
    pd_rs,
    near,
):
    bits = (b1, b2, b3, b4)
    halos = (h1, h2, h3, h4)
    me = lax.axis_index("rows")
    dp = lax.axis_index("dp")
    my_y = dp // nz
    my_z = dp % nz
    is_first = me == 0
    is_last = me == nr - 1

    def row_peer(d):
        return lax.rem(me + d, nr)

    def dp_peer(d):
        return lax.rem(my_y + d // nz, ny) * nz + lax.rem(my_z + d % nz, nz)

    def away(d, n):
        return min(d, n - d)

    far_rows = sorted(range(1, nr), key=lambda d: (-away(d, nr), d))
    far_dp = sorted(
        range(1, ny * nz), key=lambda d: (-away(d // nz, ny) - away(d % nz, nz), d)
    )
    steps = [] if nz == 1 else [1, nz - 1]
    steps = steps + ([] if ny == 1 else [nz, (ny - 1) * nz])

    barrier = pltpu.get_barrier_semaphore()
    for d in range(1, nr):
        pl.semaphore_signal(barrier, inc=1, device_id={"rows": row_peer(d)}, device_id_type=MESH)
    for d in steps:
        pl.semaphore_signal(barrier, inc=1, device_id={"dp": dp_peer(d)}, device_id_type=MESH)

    def near_send():
        for n, d in enumerate(steps):
            pl.semaphore_signal(
                near.at[n], inc=1, device_id={"dp": dp_peer(d)}, device_id_type=MESH
            )

    def near_wait():
        for n in range(len(steps)):
            pl.semaphore_wait(near.at[n], 1)

    hbm = (lat_in, b1_in, w_in_in, w_out_in, w_mid_in, b2_in, b3_in, b4_in)
    local = (lat, b1, w_in, w_out, w_mid, b2, b3, b4)

    def fetch(n):
        return pltpu.make_async_copy(hbm[n], local[n], in_sem.at[n])

    for n in range(8):
        fetch(n).start()

    def halo_copy(level, side):
        count = ROWS // FACTORS[level]
        keep = HALO[level]
        if side == 0:
            src = bits[level].at[0, pl.ds(count - keep, keep)]
            target = me + 1
        else:
            src = bits[level].at[0, pl.ds(0, keep)]
            target = me - 1
        return pltpu.make_async_remote_copy(
            src_ref=src,
            dst_ref=halos[level].at[side],
            send_sem=halo_ss.at[level, side],
            recv_sem=halo_rs.at[level, side],
            device_id={"rows": target},
            device_id_type=MESH,
        )

    def halo_send(level):
        @pl.when(jnp.logical_not(is_last))
        def _():
            halo_copy(level, 0).start()

        @pl.when(jnp.logical_not(is_first))
        def _():
            halo_copy(level, 1).start()

    def halo_wait(level):
        @pl.when(jnp.logical_not(is_first))
        def _():
            halo_copy(level, 0).wait_recv()

        @pl.when(jnp.logical_not(is_last))
        def _():
            halo_copy(level, 1).wait_recv()

    def halo_drain(level):
        @pl.when(jnp.logical_not(is_last))
        def _():
            halo_copy(level, 0).wait_send()

        @pl.when(jnp.logical_not(is_first))
        def _():
            halo_copy(level, 1).wait_send()

    def mag_copy(level, d, slot):
        return pltpu.make_async_remote_copy(
            src_ref=mags.at[level, slot],
            dst_ref=mags.at[level, slot],
            send_sem=mag_ss.at[level, d],
            recv_sem=mag_rs.at[level, slot],
            device_id={"rows": row_peer(d)},
            device_id_type=MESH,
        )

    def stage_copy(buf, ss, rs, d, slot, target):
        return pltpu.make_async_remote_copy(
            src_ref=buf.at[slot],
            dst_ref=buf.at[slot],
            send_sem=ss.at[d],
            recv_sem=rs.at[slot],
            device_id=target,
            device_id_type=MESH,
        )

    def r_copy(d, slot):
        return stage_copy(part_r, pr_ss, pr_rs, d, slot, {"rows": row_peer(d)})

    def d_copy(d, slot):
        return stage_copy(part_d, pd_ss, pd_rs, d, slot, {"dp": dp_peer(d)})

    def residual_row(level, row):
        if level == 0:
            return lat[0, row]
        return lat[0, row] - recon[0, row]

    def coarse_stage(level):
        factor = FACTORS[level]
        count = ROWS // factor
        total = jnp.zeros((CH, W), F32)
        for i in range(count):
            acc = residual_row(level, i * factor)
            for j in range(1, factor):
                acc = acc + residual_row(level, i * factor + j)
            acc = block_mean(acc, factor)
            cs[i] = acc
            total = total + jnp.abs(acc)
        summed = jnp.sum(total, axis=1, keepdims=True)
        shape = (CH, W)
        row = jnp.sum(
            jnp.where(lanes(shape) == subs(shape), jnp.broadcast_to(summed, shape), 0.0),
            axis=0,
            keepdims=True,
        )
        mags[level, me] = row

    def mag_send(level):
        for d in far_rows:
            mag_copy(level, d, me).start()

    def mag_wait(level):
        for d in range(1, nr):
            mag_copy(level, d, row_peer(d)).wait_recv()
        factor = FACTORS[level]
        side = W // factor
        row = mags[level, 0]
        for j in range(1, nr):
            row = row + mags[level, j]
        shape = (CH, W)
        spread = jnp.where(lanes(shape) == subs(shape), jnp.broadcast_to(row, shape), 0.0)
        return jnp.sum(spread, axis=1, keepdims=True) * (1.0 / (factor * side * side))

    def stats_stage(level):
        factor = FACTORS[level]
        count = ROWS // factor
        entropy = jnp.zeros((8, W), F32)
        for i in range(count):
            logits = (SHARPNESS * factor) * cs[i]
            size = jnp.abs(logits)
            small = jnp.exp(-size)
            inverse = 1.0 / (1.0 + small)
            rest = small * inverse
            each = jnp.log1p(small) + size * rest
            entropy = entropy + (each[0:8] + each[8:16]) + (each[16:24] + each[24:32])
            positive = logits >= 0.0
            ps[i] = jnp.where(positive, inverse, rest)
            qs[i] = jnp.where(positive, rest, inverse)
        sums = [jnp.zeros((8, W), F32) for _ in range(16)]
        for i in range(count):
            one = [ps[i, pl.ds(k, 8, stride=4)] for k in range(4)]
            zero = [qs[i, pl.ds(k, 8, stride=4)] for k in range(4)]
            front = [x * y for x in (zero[0], one[0]) for y in (zero[1], one[1])]
            back = [x * y for x in (zero[2], one[2]) for y in (zero[3], one[3])]
            for j in range(16):
                sums[j] = sums[j] + front[j // 4] * back[j % 4]
        lane = lanes((8, W))
        place = lane - 16 * subs((8, W))
        tile = jnp.zeros((8, W), F32)
        for j in range(16):
            tile = tile + jnp.where(place == j, jnp.sum(sums[j], axis=1, keepdims=True), 0.0)
        st[level] = jnp.sum(tile, axis=0, keepdims=True)
        flat = jnp.sum(
            jnp.where(lane == level, jnp.sum(entropy, axis=1, keepdims=True), 0.0),
            axis=0,
            keepdims=True,
        )
        st[4] = flat if level == 0 else st[4] + flat

    def spread_stage(level):
        factor = FACTORS[level]
        count = ROWS // factor
        keep = HALO[level]
        side = W // factor
        ref = bits[level]
        top = halos[level][0]
        bottom = halos[level][1]
        plane = (side, CH) if level == 0 else (CH, side)
        own_top = jnp.broadcast_to(ref[0, 0][None], (keep, *plane))
        own_bottom = jnp.broadcast_to(ref[0, count - 1][None], (keep, *plane))
        top = jnp.where(is_first, own_top, top)
        bottom = jnp.where(is_last, own_bottom, bottom)
        if factor == 1:
            for u in range(3):
                ub[u] = top[u].astype(F32)
                ub[ROWS + 3 + u] = bottom[u].astype(F32)
            for u in range(ROWS):
                ub[u + 3] = ref[0, u].astype(F32)
            return
        stack = jnp.concatenate([top, ref[0], bottom], axis=0).astype(F32).astype(BF16)
        table = column_table(side, factor)
        if level == 0:
            wide = [
                lax.dot_general(
                    stack[n], table, (((0,), (0,)), ((), ())), preferred_element_type=F32
                )
                for n in range(count + 2 * keep)
            ]
        else:
            stack = stack.reshape((count + 2 * keep) * CH, side)
            wide = jnp.dot(stack, table, preferred_element_type=F32)
            wide = wide.reshape(count + 2 * keep, CH, W)
        for u in range(ROWS + 6):
            numerator = 2 * (u - 3) + 1 - factor
            lower = numerator // (2 * factor)
            fraction = (numerator - 2 * factor * lower) / (2.0 * factor)
            at = lower + keep
            ub[u] = (1.0 - fraction) * wide[at] + fraction * wide[at + 1]

    def scale_row(u):
        low, high = side_masks(BF16)
        up = ub[u] * mg[...]
        if u < 3:
            up = up * jnp.where(is_first, 0.0, 1.0)
        elif u >= ROWS + 3:
            up = up * jnp.where(is_last, 0.0, 1.0)
        else:
            recon[0, u - 3] = recon[0, u - 3] + up
        half = up.astype(BF16)
        xs[u, 0:CH] = from_left(half, low)
        xs[u, CH : 2 * CH] = half
        xs[u, 2 * CH : 3 * CH] = from_right(half, high)

    def window(ref, row):
        a = ref[row : row + 3]
        b = ref[row + 1 : row + 4]
        depth = 3 * a.shape[1]
        return jnp.concatenate([a.reshape(depth, W), b.reshape(depth, W)], axis=1)

    def first_pair(p):
        low, high = side_masks(BF16)
        size = HID // CUTS
        for n in range(CUTS):
            at = n * size
            z = twice_gelu(
                jnp.dot(w1[at : at + size, :], window(xs, 2 * p), preferred_element_type=F32)
            )
            if p == 0:
                z = z * jnp.where(is_first, 0.0, 1.0)
            if p == PAIRS + 1:
                z = z * jnp.where(is_last, 0.0, 1.0)
            z = z.astype(BF16)
            for h in range(2):
                x = z[:, h * W : (h + 1) * W]
                fs[2 * p + h, at : at + size] = from_left(x, low)
                fs[2 * p + h, HID + at : HID + at + size] = x
                fs[2 * p + h, 2 * HID + at : 2 * HID + at + size] = from_right(x, high)

    def second_pair(p):
        cuts = 2 if p in SPLIT else 1
        size = HID // cuts
        for n in range(cuts):
            at = n * size
            z = twice_gelu(
                jnp.dot(w2[at : at + size, :], window(fs, 2 * p), preferred_element_type=F32)
            )
            for h in range(2):
                x = z[:, h * W : (h + 1) * W]
                if p == 0 and h == 0:
                    x = x * jnp.where(is_first, 0.0, 1.0)
                if p == PAIRS and h == 1:
                    x = x * jnp.where(is_last, 0.0, 1.0)
                gs[2 * p + h, at : at + size] = x.astype(BF16)

    def third_pair(p):
        low, high = side_masks(F32)
        z = jnp.dot(w3[...], window(gs, 2 * p), preferred_element_type=F32)
        for h in range(2):
            x = z[:, h * W : (h + 1) * W]
            recon[0, 2 * p + h] = recon[0, 2 * p + h] + (
                x[CH : 2 * CH] + from_left(x[0:CH], low) + from_right(x[2 * CH : 3 * CH], high)
            )

    fetch(0).wait()
    coarse_stage(0)
    pl.semaphore_wait(barrier, nr - 1 + len(steps))
    mag_send(0)
    near_send()
    fetch(1).wait()
    halo_send(0)
    for n in (5, 6, 7):
        fetch(n).wait()
    for level in range(1, 4):
        halo_send(level)

    for n in (2, 3, 4):
        fetch(n).wait()
    w1[...] = w_in[...].reshape(9 * CH, HID).T
    for dr in range(3):
        for dc in range(3):
            w3[dc * CH : (dc + 1) * CH, dr * HID : (dr + 1) * HID] = w_out[dr, dc] * 0.5
    for tap in range(9):
        w2[:, tap * HID : (tap + 1) * HID] = (w_mid[tap // 3, tap % 3] * 0.5).T
    recon[...] = jnp.zeros_like(recon)

    def one_level(level, _):
        for k in range(4):

            @pl.when(level == k)
            def _(k=k):
                if k > 0:
                    coarse_stage(k)
                if k == 3:
                    stats_stage(k)
                    part_r[me] = st[...]
                    for d in far_rows:
                        r_copy(d, me).start()
                if k > 0:
                    mag_send(k)
                if k < 3:
                    stats_stage(k)
                halo_wait(k)
                spread_stage(k)
                if k > 0:
                    halo_drain(k - 1)
                    for d in range(1, nr):
                        mag_copy(k - 1, d, me).wait_send()
                if k < 3:
                    near_wait()
                if k < 2:
                    near_send()
                if k == 3:
                    for d in range(1, nr):
                        r_copy(d, row_peer(d)).wait_recv()
                    total = part_r[0]
                    for j in range(1, nr):
                        total = total + part_r[j]
                    part_d[dp] = total
                    for d in far_dp:
                        d_copy(d, dp).start()
                mg[...] = jnp.broadcast_to(mag_wait(k), (CH, W))
                if k < 2:
                    near_wait()
                    near_send()

        for u in range(ROWS + 6):
            scale_row(u)
        for p in range(PAIRS + 5):
            if p < PAIRS + 2:
                first_pair(p)
            if 3 <= p < PAIRS + 4:
                second_pair(p - 3)
            if p >= 5:
                third_pair(p - 5)
        return 0

    lax.fori_loop(0, 4, one_level, 0)

    copy_out = pltpu.make_async_copy(recon, recon_out, out_sem)
    copy_out.start()
    halo_drain(3)
    for d in range(1, nr):
        mag_copy(3, d, me).wait_send()
    for d in range(1, nr):
        r_copy(d, me).wait_send()
    for d in range(1, ny * nz):
        d_copy(d, dp).wait_send()
    copy_out.wait()
    for d in range(1, ny * nz):
        d_copy(d, dp_peer(d)).wait_recv()
    total = part_d[0]
    for j in range(1, ny * nz):
        total = total + part_d[j]
    final[...] = total


def finish(
    images, recon_in, sums, recon, uent_out, sent_out, buf, uent, sent, in_sem, out_sem, small
):
    part = ROWS // PARTS

    def inward(n):
        at = pl.ds(n * part, part)
        return pltpu.make_async_copy(recon_in.at[0, at], buf.at[at], in_sem.at[n])

    def outward(n):
        at = pl.ds(n * part, part)
        return pltpu.make_async_copy(buf.at[at], recon.at[0, at], out_sem.at[n])

    for n in range(PARTS):
        inward(n).start()
    for level in range(4):
        side = W // FACTORS[level]
        usage = sums[level] * (1.0 / (images * side * side * FACTORS[level]))
        terms = -(usage * jnp.log(usage + EPSILON))
        shape = (W, 8)
        group = subs(shape) // 16
        pick = jnp.where(group == lanes(shape), 1.0, 0.0)
        uent[level : level + 1, :] = jnp.dot(
            terms, pick, precision=lax.Precision.HIGHEST, preferred_element_type=F32
        )
    lane = lanes((1, W))
    scale = jnp.zeros((1, W), F32)
    for level in range(4):
        side = W // FACTORS[level]
        scale = jnp.where(
            lane == level, 1.0 / (images * side * side * FACTORS[level] * CH), scale
        )
    sent[...] = (sums[4] * scale)[:, 0:4]
    pairs = (
        pltpu.make_async_copy(uent, uent_out, small.at[0]),
        pltpu.make_async_copy(sent, sent_out, small.at[1]),
    )
    for n in range(PARTS):
        inward(n).wait()
        outward(n).start()
    for copy in pairs:
        copy.start()
    for copy in pairs:
        copy.wait()
    for n in range(PARTS):
        outward(n).wait()


def solution(mesh):
    nd = mesh.shape["dp"]
    nr = mesh.shape["rows"]
    ny = 4 if nd % 4 == 0 and nd >= 16 else 1
    nz = nd // ny

    vmem = pl.BlockSpec(memory_space=pltpu.VMEM)
    dma = pltpu.SemaphoreType.DMA

    def on_device(lat, b1, *rest):
        anywhere = pl.BlockSpec(memory_space=pl.ANY)
        recon, sums = pl.pallas_call(
            functools.partial(body, ny, nz, nr),
            out_shape=(
                jax.ShapeDtypeStruct((1, ROWS, CH, W), F32),
                jax.ShapeDtypeStruct((5, 1, W), F32),
            ),
            in_specs=[pl.BlockSpec(memory_space=pltpu.HBM)] * 8,
            out_specs=(anywhere, vmem),
            scratch_shapes=[
                pltpu.VMEM((1, ROWS, CH, W), F32),
                pltpu.VMEM((1, ROWS, CH, W), F32),
                pltpu.VMEM((1, 2, 16, CH), jnp.int32),
                pltpu.VMEM((1, 4, CH, 32), jnp.int32),
                pltpu.VMEM((1, 8, CH, 64), jnp.int32),
                pltpu.VMEM((1, ROWS, CH, W), jnp.int32),
                pltpu.VMEM((3, 3, CH, HID), BF16),
                pltpu.VMEM((3, 3, HID, HID), BF16),
                pltpu.VMEM((3, 3, CH, HID), BF16),
                pltpu.VMEM((HID, 9 * CH), BF16),
                pltpu.VMEM((HID, 9 * HID), BF16),
                pltpu.VMEM((3 * CH, 3 * HID), BF16),
                pltpu.VMEM((ROWS + 6, 3 * CH, W), BF16),
                pltpu.VMEM((ROWS + 4, 3 * HID, W), BF16),
                pltpu.VMEM((ROWS + 2, HID, W), BF16),
                pltpu.VMEM((ROWS + 6, CH, W), F32),
                pltpu.VMEM((ROWS, CH, W), F32),
                pltpu.VMEM((ROWS, CH, W), F32),
                pltpu.VMEM((ROWS, CH, W), F32),
                pltpu.VMEM((2, HALO[0], 16, CH), jnp.int32),
                pltpu.VMEM((2, HALO[1], CH, 32), jnp.int32),
                pltpu.VMEM((2, HALO[2], CH, 64), jnp.int32),
                pltpu.VMEM((2, HALO[3], CH, 128), jnp.int32),
                pltpu.VMEM((4, nr, 1, W), F32),
                pltpu.VMEM((CH, W), F32),
                pltpu.VMEM((5, 1, W), F32),
                pltpu.VMEM((nr, 5, 1, W), F32),
                pltpu.VMEM((nd, 5, 1, W), F32),
                dma((8,)),
                dma,
                dma((4, 2)),
                dma((4, 2)),
                dma((4, nr)),
                dma((4, nr)),
                dma((nr,)),
                dma((nr,)),
                dma((nd,)),
                dma((nd,)),
                pltpu.SemaphoreType.REGULAR((4,)),
            ],
            compiler_params=pltpu.CompilerParams(
                collective_id=0, has_side_effects=True, vmem_limit_bytes=VMEM_LIMIT
            ),
        )(lat, jnp.swapaxes(b1, 2, 3), *rest)
        recon, uent, sent = pl.pallas_call(
            functools.partial(finish, nd),
            out_shape=(
                jax.ShapeDtypeStruct((1, ROWS, CH, W), F32),
                jax.ShapeDtypeStruct((4, 8), F32),
                jax.ShapeDtypeStruct((1, 4), F32),
            ),
            in_specs=[anywhere, vmem],
            out_specs=(anywhere, anywhere, anywhere),
            scratch_shapes=[
                pltpu.VMEM((ROWS, CH, W), F32),
                pltpu.VMEM((4, 8), F32),
                pltpu.VMEM((1, 4), F32),
                dma((PARTS,)),
                dma((PARTS,)),
                dma((2,)),
            ],
            compiler_params=pltpu.CompilerParams(vmem_limit_bytes=VMEM_LIMIT),
        )(recon, sums)
        return recon, uent, sent.reshape(4)

    split = P("dp", "rows", None, None)
    return jax.shard_map(
        on_device,
        mesh=mesh,
        in_specs=(split,) * 5 + (P(),) * 3,
        out_specs=(split, P(), P()),
        check_vma=False,
    )
```

```python
import functools

import jax
import jax.numpy as jnp
from jax import lax
from jax.experimental import pallas as pl
from jax.experimental.pallas import tpu as pltpu
from jax.sharding import PartitionSpec as P

MESH = pl.DeviceIdType.MESH
F32 = jnp.float32
BF16 = jnp.bfloat16
FACTORS = (8, 4, 2, 1)
HALO = (1, 2, 2, 3)
SHARPNESS = 2.0
EPSILON = 1e-6
VMEM_LIMIT = 56280000
ROWS = 16
CH = 32
HID = 256
W = 128
PAIRS = ROWS // 2
CUTS = 2
SPLIT = tuple(range(PAIRS + 1))


def lanes(shape):
    return lax.broadcasted_iota(jnp.int32, shape, len(shape) - 1)


def subs(shape):
    return lax.broadcasted_iota(jnp.int32, shape, len(shape) - 2)


def side_masks(dtype):
    lane = lanes((1, W))
    low = jnp.where(lane == 0, 0.0, 1.0).astype(dtype)
    high = jnp.where(lane == W - 1, 0.0, 1.0).astype(dtype)
    return low, high


def from_left(x, low):
    return pltpu.roll(x, 1, 1) * low


def from_right(x, high):
    return pltpu.roll(x, W - 1, 1) * high


def twice_gelu(x):
    inner = x * (0.7978845608028654 + (0.7978845608028654 * 0.044715) * (x * x))
    return x + x * jnp.tanh(inner)


def block_mean(x, factor):
    lane = lanes(x.shape)
    step = 1
    while step < factor:
        below = pltpu.roll(x, step, 1)
        above = pltpu.roll(x, W - step, 1)
        x = x + jnp.where((lane & step) == 0, above, below)
        step *= 2
    return x * (1.0 / (factor * factor))


def column_table(side, factor):
    shape = (side, W)
    target = lanes(shape)
    row = subs(shape)
    shift = (2 * factor).bit_length() - 1
    numerator = 2 * target + 1 - factor
    lower = lax.shift_right_arithmetic(numerator, jnp.full(shape, shift, jnp.int32))
    fraction = (numerator - 2 * factor * lower).astype(F32) * (1.0 / (2.0 * factor))
    low_at = jnp.clip(lower, 0, side - 1)
    high_at = jnp.clip(lower + 1, 0, side - 1)
    table = jnp.where(row == low_at, 1.0 - fraction, 0.0) + jnp.where(
        row == high_at, fraction, 0.0
    )
    return table.astype(BF16)


def body(ny, nz, nr, pieces, *refs):
    (
        lat_in,
        b1_in,
        b2_in,
        b3_in,
        b4_in,
        w_in_in,
        w_mid_in,
        w_out_in,
    ) = refs[:8]
    recon_out = refs[8 : 8 + pieces]
    (
        final,
        recon,
        lat,
        b1,
        b2,
        b3,
        b4,
        w_in,
        w_mid,
        w_out,
        w1,
        w2,
        w3,
        xs,
        fs,
        gs,
        ub,
        cs,
        ps,
        qs,
        h1,
        h2,
        h3,
        h4,
        mags,
        mg,
        st,
        part_r,
        part_d,
        in_sem,
        halo_ss,
        halo_rs,
        mag_ss,
        mag_rs,
        pr_ss,
        pr_rs,
        pd_ss,
        pd_rs,
        near,
    ) = refs[8 + pieces :]
    bits = (b1, b2, b3, b4)
    halos = (h1, h2, h3, h4)
    me = lax.axis_index("rows")
    dp = lax.axis_index("dp")
    my_y = dp // nz
    my_z = dp % nz
    is_first = me == 0
    is_last = me == nr - 1

    def row_peer(d):
        return lax.rem(me + d, nr)

    def dp_peer(d):
        return lax.rem(my_y + d // nz, ny) * nz + lax.rem(my_z + d % nz, nz)

    def away(d, n):
        return min(d, n - d)

    far_rows = sorted(range(1, nr), key=lambda d: (-away(d, nr), d))
    far_dp = sorted(
        range(1, ny * nz), key=lambda d: (-away(d // nz, ny) - away(d % nz, nz), d)
    )
    steps = [] if nz == 1 else [1, nz - 1]
    steps = steps + ([] if ny == 1 else [nz, (ny - 1) * nz])

    barrier = pltpu.get_barrier_semaphore()
    for d in range(1, nr):
        pl.semaphore_signal(barrier, inc=1, device_id={"rows": row_peer(d)}, device_id_type=MESH)
    for d in steps:
        pl.semaphore_signal(barrier, inc=1, device_id={"dp": dp_peer(d)}, device_id_type=MESH)

    def near_send():
        for n, d in enumerate(steps):
            pl.semaphore_signal(
                near.at[n], inc=1, device_id={"dp": dp_peer(d)}, device_id_type=MESH
            )

    def near_wait():
        for n in range(len(steps)):
            pl.semaphore_wait(near.at[n], 1)

    hbm = (lat_in, b1_in, w_in_in, w_out_in, w_mid_in, b2_in, b3_in, b4_in)
    local = (lat, b1, w_in, w_out, w_mid, b2, b3, b4)

    def fetch(n):
        return pltpu.make_async_copy(hbm[n], local[n], in_sem.at[n])

    for n in range(8):
        fetch(n).start()

    def halo_copy(level, side):
        count = ROWS // FACTORS[level]
        keep = HALO[level]
        if side == 0:
            src = bits[level].at[0, pl.ds(count - keep, keep)]
            target = me + 1
        else:
            src = bits[level].at[0, pl.ds(0, keep)]
            target = me - 1
        return pltpu.make_async_remote_copy(
            src_ref=src,
            dst_ref=halos[level].at[side],
            send_sem=halo_ss.at[level, side],
            recv_sem=halo_rs.at[level, side],
            device_id={"rows": target},
            device_id_type=MESH,
        )

    def halo_send(level):
        @pl.when(jnp.logical_not(is_last))
        def _():
            halo_copy(level, 0).start()

        @pl.when(jnp.logical_not(is_first))
        def _():
            halo_copy(level, 1).start()

    def halo_wait(level):
        @pl.when(jnp.logical_not(is_first))
        def _():
            halo_copy(level, 0).wait_recv()

        @pl.when(jnp.logical_not(is_last))
        def _():
            halo_copy(level, 1).wait_recv()

    def halo_drain(level):
        @pl.when(jnp.logical_not(is_last))
        def _():
            halo_copy(level, 0).wait_send()

        @pl.when(jnp.logical_not(is_first))
        def _():
            halo_copy(level, 1).wait_send()

    def mag_copy(level, d, slot):
        return pltpu.make_async_remote_copy(
            src_ref=mags.at[level, slot],
            dst_ref=mags.at[level, slot],
            send_sem=mag_ss.at[level, d],
            recv_sem=mag_rs.at[level, slot],
            device_id={"rows": row_peer(d)},
            device_id_type=MESH,
        )

    def stage_copy(buf, ss, rs, d, slot, target):
        return pltpu.make_async_remote_copy(
            src_ref=buf.at[slot],
            dst_ref=buf.at[slot],
            send_sem=ss.at[d],
            recv_sem=rs.at[slot],
            device_id=target,
            device_id_type=MESH,
        )

    def r_copy(d, slot):
        return stage_copy(part_r, pr_ss, pr_rs, d, slot, {"rows": row_peer(d)})

    def d_copy(d, slot):
        return stage_copy(part_d, pd_ss, pd_rs, d, slot, {"dp": dp_peer(d)})

    def summed(ref, count):
        parts = [ref[j] for j in range(count)]
        while len(parts) > 1:
            rest = [parts[-1]] if len(parts) % 2 else []
            parts = [a + b for a, b in zip(parts[0::2], parts[1::2])] + rest
        return parts[0]

    def residual_row(level, row):
        if level == 0:
            return lat[0, row]
        return lat[0, row] - recon[0, row]

    def coarse_stage(level):
        factor = FACTORS[level]
        count = ROWS // factor
        total = jnp.zeros((CH, W), F32)
        for i in range(count):
            acc = residual_row(level, i * factor)
            for j in range(1, factor):
                acc = acc + residual_row(level, i * factor + j)
            acc = block_mean(acc, factor)
            cs[i] = acc
            total = total + jnp.abs(acc)
        summed = jnp.sum(total, axis=1, keepdims=True)
        shape = (CH, W)
        row = jnp.sum(
            jnp.where(lanes(shape) == subs(shape), jnp.broadcast_to(summed, shape), 0.0),
            axis=0,
            keepdims=True,
        )
        mags[level, me] = row

    def mag_send(level):
        for d in far_rows:
            mag_copy(level, d, me).start()

    def mag_wait(level):
        for d in range(1, nr):
            mag_copy(level, d, row_peer(d)).wait_recv()
        factor = FACTORS[level]
        side = W // factor
        row = summed(mags.at[level], nr)
        shape = (CH, W)
        spread = jnp.where(lanes(shape) == subs(shape), jnp.broadcast_to(row, shape), 0.0)
        return jnp.sum(spread, axis=1, keepdims=True) * (1.0 / (factor * side * side))

    def stats_stage(level):
        factor = FACTORS[level]
        count = ROWS // factor
        entropy = jnp.zeros((8, W), F32)
        for i in range(count):
            logits = (SHARPNESS * factor) * cs[i]
            size = jnp.abs(logits)
            small = jnp.exp(-size)
            inverse = 1.0 / (1.0 + small)
            rest = small * inverse
            each = jnp.log1p(small) + size * rest
            entropy = entropy + (each[0:8] + each[8:16]) + (each[16:24] + each[24:32])
            positive = logits >= 0.0
            ps[i] = jnp.where(positive, inverse, rest)
            qs[i] = jnp.where(positive, rest, inverse)
        sums = [jnp.zeros((8, W), F32) for _ in range(16)]
        for i in range(count):
            one = [ps[i, pl.ds(k, 8, stride=4)] for k in range(4)]
            zero = [qs[i, pl.ds(k, 8, stride=4)] for k in range(4)]
            front = [x * y for x in (zero[0], one[0]) for y in (zero[1], one[1])]
            back = [x * y for x in (zero[2], one[2]) for y in (zero[3], one[3])]
            for j in range(16):
                sums[j] = sums[j] + front[j // 4] * back[j % 4]
        lane = lanes((8, W))
        place = lane - 16 * subs((8, W))
        tile = jnp.zeros((8, W), F32)
        for j in range(16):
            tile = tile + jnp.where(place == j, jnp.sum(sums[j], axis=1, keepdims=True), 0.0)
        st[level] = jnp.sum(tile, axis=0, keepdims=True)
        flat = jnp.sum(
            jnp.where(lane == level, jnp.sum(entropy, axis=1, keepdims=True), 0.0),
            axis=0,
            keepdims=True,
        )
        st[4] = flat if level == 0 else st[4] + flat

    def spread_stage(level):
        factor = FACTORS[level]
        count = ROWS // factor
        keep = HALO[level]
        side = W // factor
        ref = bits[level]
        top = halos[level][0]
        bottom = halos[level][1]
        plane = (side, CH) if level == 0 else (CH, side)
        own_top = jnp.broadcast_to(ref[0, 0][None], (keep, *plane))
        own_bottom = jnp.broadcast_to(ref[0, count - 1][None], (keep, *plane))
        top = jnp.where(is_first, own_top, top)
        bottom = jnp.where(is_last, own_bottom, bottom)
        if factor == 1:
            for u in range(3):
                ub[u] = top[u].astype(F32)
                ub[ROWS + 3 + u] = bottom[u].astype(F32)
            for u in range(ROWS):
                ub[u + 3] = ref[0, u].astype(F32)
            return
        stack = jnp.concatenate([top, ref[0], bottom], axis=0).astype(F32).astype(BF16)
        table = column_table(side, factor)
        if level == 0:
            wide = [
                lax.dot_general(
                    stack[n], table, (((0,), (0,)), ((), ())), preferred_element_type=F32
                )
                for n in range(count + 2 * keep)
            ]
        else:
            stack = stack.reshape((count + 2 * keep) * CH, side)
            wide = jnp.dot(stack, table, preferred_element_type=F32)
            wide = wide.reshape(count + 2 * keep, CH, W)
        for u in range(ROWS + 6):
            numerator = 2 * (u - 3) + 1 - factor
            lower = numerator // (2 * factor)
            fraction = (numerator - 2 * factor * lower) / (2.0 * factor)
            at = lower + keep
            ub[u] = (1.0 - fraction) * wide[at] + fraction * wide[at + 1]

    def scale_row(u):
        low, high = side_masks(BF16)
        up = ub[u] * mg[...]
        if u < 3:
            up = up * jnp.where(is_first, 0.0, 1.0)
        elif u >= ROWS + 3:
            up = up * jnp.where(is_last, 0.0, 1.0)
        else:
            recon[0, u - 3] = recon[0, u - 3] + up
        half = up.astype(BF16)
        xs[u, 0:CH] = from_left(half, low)
        xs[u, CH : 2 * CH] = half
        xs[u, 2 * CH : 3 * CH] = from_right(half, high)

    def window(ref, row):
        a = ref[row : row + 3]
        b = ref[row + 1 : row + 4]
        depth = 3 * a.shape[1]
        return jnp.concatenate([a.reshape(depth, W), b.reshape(depth, W)], axis=1)

    def first_pair(p):
        low, high = side_masks(BF16)
        size = HID // CUTS
        for n in range(CUTS):
            at = n * size
            z = twice_gelu(
                jnp.dot(w1[at : at + size, :], window(xs, 2 * p), preferred_element_type=F32)
            )
            if p == 0:
                z = z * jnp.where(is_first, 0.0, 1.0)
            if p == PAIRS + 1:
                z = z * jnp.where(is_last, 0.0, 1.0)
            z = z.astype(BF16)
            for h in range(2):
                x = z[:, h * W : (h + 1) * W]
                fs[2 * p + h, at : at + size] = from_left(x, low)
                fs[2 * p + h, HID + at : HID + at + size] = x
                fs[2 * p + h, 2 * HID + at : 2 * HID + at + size] = from_right(x, high)

    def second_pair(p):
        cuts = 2 if p in SPLIT else 1
        size = HID // cuts
        for n in range(cuts):
            at = n * size
            z = twice_gelu(
                jnp.dot(w2[at : at + size, :], window(fs, 2 * p), preferred_element_type=F32)
            )
            for h in range(2):
                x = z[:, h * W : (h + 1) * W]
                if p == 0 and h == 0:
                    x = x * jnp.where(is_first, 0.0, 1.0)
                if p == PAIRS and h == 1:
                    x = x * jnp.where(is_last, 0.0, 1.0)
                gs[2 * p + h, at : at + size] = x.astype(BF16)

    def third_pair(p):
        low, high = side_masks(F32)
        z = jnp.dot(w3[...], window(gs, 2 * p), preferred_element_type=F32)
        for h in range(2):
            x = z[:, h * W : (h + 1) * W]
            recon[0, 2 * p + h] = recon[0, 2 * p + h] + (
                x[CH : 2 * CH] + from_left(x[0:CH], low) + from_right(x[2 * CH : 3 * CH], high)
            )

    fetch(0).wait()
    coarse_stage(0)
    pl.semaphore_wait(barrier, nr - 1 + len(steps))
    mag_send(0)
    near_send()
    fetch(1).wait()
    halo_send(0)
    for n in (5, 6, 7):
        fetch(n).wait()
    for level in range(1, 4):
        halo_send(level)

    for n in (2, 3, 4):
        fetch(n).wait()
    w1[...] = w_in[...].reshape(9 * CH, HID).T
    for dr in range(3):
        for dc in range(3):
            w3[dc * CH : (dc + 1) * CH, dr * HID : (dr + 1) * HID] = w_out[dr, dc] * 0.5
    for tap in range(9):
        w2[:, tap * HID : (tap + 1) * HID] = (w_mid[tap // 3, tap % 3] * 0.5).T
    recon[...] = jnp.zeros_like(recon)

    def one_level(level, _):
        for k in range(4):

            @pl.when(level == k)
            def _(k=k):
                if k > 0:
                    coarse_stage(k)
                if k == 3:
                    stats_stage(k)
                    part_r[me] = st[...]
                    for d in far_rows:
                        r_copy(d, me).start()
                if k > 0:
                    mag_send(k)
                if k < 3:
                    stats_stage(k)
                halo_wait(k)
                spread_stage(k)
                if k > 0:
                    halo_drain(k - 1)
                    for d in range(1, nr):
                        mag_copy(k - 1, d, me).wait_send()
                if k < 3:
                    near_wait()
                if k < 2:
                    near_send()
                if k == 3:
                    for d in range(1, nr):
                        r_copy(d, row_peer(d)).wait_recv()
                    part_d[dp] = summed(part_r, nr)
                    for d in far_dp:
                        d_copy(d, dp).start()
                mg[...] = jnp.broadcast_to(mag_wait(k), (CH, W))
                if k < 2:
                    near_wait()
                    near_send()

        for u in range(ROWS + 6):
            scale_row(u)
        for p in range(PAIRS + 5):
            if p < PAIRS + 2:
                first_pair(p)
            if 3 <= p < PAIRS + 4:
                second_pair(p - 3)
            if p >= 5:
                third_pair(p - 5)
        return 0

    lax.fori_loop(0, 4, one_level, 0)

    for n in range(ROWS):
        recon_out[n][...] = recon[0, n]
    halo_drain(3)
    for d in range(1, nr):
        mag_copy(3, d, me).wait_send()
    for d in range(1, nr):
        r_copy(d, me).wait_send()
    for d in range(1, ny * nz):
        d_copy(d, dp).wait_send()
    for d in reversed(far_dp):
        d_copy(d, dp_peer(d)).wait_recv()
    final[...] = summed(part_d, ny * nz)


def finish(images, *refs):
    rows = refs[:ROWS]
    sums, recon, uent_out, sent_out, uent, sent, out_sem, small = refs[ROWS:]

    def outward(n):
        return pltpu.make_async_copy(rows[n], recon.at[0, n], out_sem.at[n])

    for n in range(ROWS):
        outward(n).start()
    for level in range(4):
        side = W // FACTORS[level]
        usage = sums[level] * (1.0 / (images * side * side * FACTORS[level]))
        terms = -(usage * jnp.log(usage + EPSILON))
        shape = (W, 8)
        group = subs(shape) // 16
        pick = jnp.where(group == lanes(shape), 1.0, 0.0)
        uent[level : level + 1, :] = jnp.dot(
            terms, pick, precision=lax.Precision.HIGHEST, preferred_element_type=F32
        )
    lane = lanes((1, W))
    scale = jnp.zeros((1, W), F32)
    for level in range(4):
        side = W // FACTORS[level]
        scale = jnp.where(
            lane == level, 1.0 / (images * side * side * FACTORS[level] * CH), scale
        )
    sent[...] = (sums[4] * scale)[:, 0:4]
    pairs = (
        pltpu.make_async_copy(uent, uent_out, small.at[0]),
        pltpu.make_async_copy(sent, sent_out, small.at[1]),
    )
    for copy in pairs:
        copy.start()
    for copy in pairs:
        copy.wait()
    for n in range(ROWS):
        outward(n).wait()


def solution(mesh):
    nd = mesh.shape["dp"]
    nr = mesh.shape["rows"]
    ny = 4 if nd % 4 == 0 and nd >= 16 else 1
    nz = nd // ny

    vmem = pl.BlockSpec(memory_space=pltpu.VMEM)
    dma = pltpu.SemaphoreType.DMA

    def on_device(lat, b1, *rest):
        anywhere = pl.BlockSpec(memory_space=pl.ANY)
        *rows, sums = pl.pallas_call(
            functools.partial(body, ny, nz, nr, ROWS),
            out_shape=(
                *(jax.ShapeDtypeStruct((CH, W), F32) for _ in range(ROWS)),
                jax.ShapeDtypeStruct((5, 1, W), F32),
            ),
            in_specs=[pl.BlockSpec(memory_space=pltpu.HBM)] * 8,
            out_specs=(vmem,) * (ROWS + 1),
            scratch_shapes=[
                pltpu.VMEM((1, ROWS, CH, W), F32),
                pltpu.VMEM((1, ROWS, CH, W), F32),
                pltpu.VMEM((1, 2, 16, CH), jnp.int32),
                pltpu.VMEM((1, 4, CH, 32), jnp.int32),
                pltpu.VMEM((1, 8, CH, 64), jnp.int32),
                pltpu.VMEM((1, ROWS, CH, W), jnp.int32),
                pltpu.VMEM((3, 3, CH, HID), BF16),
                pltpu.VMEM((3, 3, HID, HID), BF16),
                pltpu.VMEM((3, 3, CH, HID), BF16),
                pltpu.VMEM((HID, 9 * CH), BF16),
                pltpu.VMEM((HID, 9 * HID), BF16),
                pltpu.VMEM((3 * CH, 3 * HID), BF16),
                pltpu.VMEM((ROWS + 6, 3 * CH, W), BF16),
                pltpu.VMEM((ROWS + 4, 3 * HID, W), BF16),
                pltpu.VMEM((ROWS + 2, HID, W), BF16),
                pltpu.VMEM((ROWS + 6, CH, W), F32),
                pltpu.VMEM((ROWS, CH, W), F32),
                pltpu.VMEM((ROWS, CH, W), F32),
                pltpu.VMEM((ROWS, CH, W), F32),
                pltpu.VMEM((2, HALO[0], 16, CH), jnp.int32),
                pltpu.VMEM((2, HALO[1], CH, 32), jnp.int32),
                pltpu.VMEM((2, HALO[2], CH, 64), jnp.int32),
                pltpu.VMEM((2, HALO[3], CH, 128), jnp.int32),
                pltpu.VMEM((4, nr, 1, W), F32),
                pltpu.VMEM((CH, W), F32),
                pltpu.VMEM((5, 1, W), F32),
                pltpu.VMEM((nr, 5, 1, W), F32),
                pltpu.VMEM((nd, 5, 1, W), F32),
                dma((8,)),
                dma((4, 2)),
                dma((4, 2)),
                dma((4, nr)),
                dma((4, nr)),
                dma((nr,)),
                dma((nr,)),
                dma((nd,)),
                dma((nd,)),
                pltpu.SemaphoreType.REGULAR((4,)),
            ],
            compiler_params=pltpu.CompilerParams(
                collective_id=0, has_side_effects=True, vmem_limit_bytes=VMEM_LIMIT
            ),
        )(lat, jnp.swapaxes(b1, 2, 3), *rest)
        recon, uent, sent = pl.pallas_call(
            functools.partial(finish, nd),
            out_shape=(
                jax.ShapeDtypeStruct((1, ROWS, CH, W), F32),
                jax.ShapeDtypeStruct((4, 8), F32),
                jax.ShapeDtypeStruct((1, 4), F32),
            ),
            in_specs=[anywhere] * ROWS + [vmem],
            out_specs=(anywhere, anywhere, anywhere),
            scratch_shapes=[
                pltpu.VMEM((4, 8), F32),
                pltpu.VMEM((1, 4), F32),
                dma((ROWS,)),
                dma((2,)),
            ],
            compiler_params=pltpu.CompilerParams(vmem_limit_bytes=VMEM_LIMIT),
        )(*rows, sums)
        return recon, uent, sent.reshape(4)

    split = P("dp", "rows", None, None)
    return jax.shard_map(
        on_device,
        mesh=mesh,
        in_specs=(split,) * 5 + (P(),) * 3,
        out_specs=(split, P(), P()),
        check_vma=False,
    )
```
